32 devices in a mesh: part: 2 (over x), col: 4 (over z), row: 4 (over y, core).
Axes of the slice: x: 2, y: 2, z: 4, core: 2. Of those that a mesh axis runs over, the one named last changes fastest.
Arguments:
- a_blocks: float32 [80, 128, 5120], P(('part', 'row'), None, 'col'), parts along dimension 0
Outputs:
- output: float32 [80, 128, 5120], P(('part', 'row'), None, 'col'), parts along dimension 0
There are 2 independent parts. The reference program is written for one: setup_inputs(seed, part) draws one part's arguments, and reference() takes and returns one part's arrays. A program takes and returns all parts, laid end to end along the dimension named above; each array names one.
All inputs are finite; a program needn't handle non-finite values.
Results may differ from the reference program's by a relative error of at most 0.001.
Values sent between devices are 32-bit elements.
A program may use at most 1 GiB of HBM per device.

```python
import jax
import jax.numpy as jnp

N = 5120
NB = 128
GRID_ROWS = 4
GRID_COLS = 4
NUM_BLOCKS = N // NB
ROW_BLOCKS = NUM_BLOCKS // GRID_ROWS
COL_BLOCKS = NUM_BLOCKS // GRID_COLS
RANK_COLS = N // 4


def to_natural(blocked):
    row_perm = blocked.reshape(GRID_ROWS, ROW_BLOCKS, NB, N).transpose(1, 0, 2, 3).reshape(N, N)
    return row_perm.reshape(N, GRID_COLS, COL_BLOCKS, NB).transpose(0, 2, 1, 3).reshape(N, N)


def to_cyclic(matrix):
    row_perm = matrix.reshape(ROW_BLOCKS, GRID_ROWS, NB, N).transpose(1, 0, 2, 3).reshape(N, N)
    return row_perm.reshape(N, COL_BLOCKS, GRID_COLS, NB).transpose(0, 2, 1, 3).reshape(NUM_BLOCKS, NB, N)


def setup_inputs(seed: int = 0, part: int = 0) -> dict:
    base_key = jax.random.fold_in(jax.random.key(seed), part)
    factor = jax.random.normal(base_key, (N, RANK_COLS), jnp.float32)
    gram_mat = jnp.dot(factor, factor.T, preferred_element_type=jnp.float32)
    spd_matrix = 0.5 * (gram_mat + gram_mat.T) / RANK_COLS + jnp.eye(N, dtype=jnp.float32)
    return {"a_blocks": to_cyclic(spd_matrix)}


def reference(a_blocks):
    lower = jnp.linalg.cholesky(to_natural(a_blocks))
    return to_cyclic(lower)
```

```python
import jax
import jax.numpy as jnp
from jax import lax
from jax.experimental import pallas as pl
from jax.experimental.pallas import tpu as pltpu
from jax.sharding import PartitionSpec as P

HI = lax.Precision.HIGHEST
MESH = pl.DeviceIdType.MESH
NB = 128
N_STEPS = 40
G = 4
PAIRS = 5
N_BLOCKS = 120


def _factor(s_val, u_ref, w_ref):
    sub = lax.broadcasted_iota(jnp.int32, (8, NB), 0)
    lane = lax.broadcasted_iota(jnp.int32, (8, NB), 1)
    rows = [s_val[8 * t:8 * t + 8, :] for t in range(16)]
    inv = [jnp.where(lane == sub + 8 * t, 1.0, 0.0) for t in range(16)]
    full = (8, NB)
    for b in range(16):
        p, q = rows[b], inv[b]
        ncol = 8 if b == 15 else 16
        cols = [jnp.broadcast_to(p[:, 8 * b + i:8 * b + i + 1], full) for i in range(ncol)]
        for j in range(8):
            rinv = lax.rsqrt(jnp.broadcast_to(cols[j][j:j + 1, :], full))
            low = jnp.where(sub > j, cols[j] * rinv, 0.0)
            prow = jnp.broadcast_to(p[j:j + 1, :], full) * rinv
            p = jnp.where(sub == j, prow, p - low * prow)
            qrow = jnp.broadcast_to(q[j:j + 1, :], full) * rinv
            q = jnp.where(sub == j, qrow, q - low * qrow)
            for i in range(j + 1, ncol):
                crow = jnp.broadcast_to(cols[i][j:j + 1, :], full) * rinv
                nxt = cols[i] - low * crow
                cols[i] = jnp.where(sub == j, crow, nxt) if i >= 8 else nxt
        u_ref[8 * b:8 * b + 8, :] = jnp.where(lane >= sub + 8 * b, p, 0.0)
        w_ref[8 * b:8 * b + 8, :] = q
        if b < 15:
            pn, qn = rows[b + 1], inv[b + 1]
            for i in range(8):
                dp = jnp.sum(cols[8 + i] * p, axis=0, keepdims=True)
                dq = jnp.sum(cols[8 + i] * q, axis=0, keepdims=True)
                pn = jnp.where(sub == i, pn - dp, pn)
                qn = jnp.where(sub == i, qn - dq, qn)
            rows[b + 1], inv[b + 1] = pn, qn
        if b < 14:
            both = jnp.concatenate([p, q], axis=1)
            upd = lax.dot_general(p, both, (((0,), (0,)), ((), ())), precision=HI, preferred_element_type=jnp.float32)
            for t in range(b + 2, 16):
                rows[t] = rows[t] - upd[8 * t:8 * t + 8, :NB]
                inv[t] = inv[t] - upd[8 * t:8 * t + 8, NB:]


def _nt(x, y):
    return lax.dot_general(x, y, (((1,), (1,)), ((), ())), precision=HI, preferred_element_type=jnp.float32)


def _div(x, n):
    return lax.div(x, jnp.int32(n))


def _rem(x, n):
    return lax.rem(x, jnp.int32(n))


def _kernel(a_hbm, o_hbm, mat, pan, wb, raw, diag, ubuf, zero,
            row_sem, col_sem, w_sem, raw_sem, send_sem, in_sem, out_sem):
    me_c = lax.axis_index("col").astype(jnp.int32)
    me_r = lax.axis_index("row").astype(jnp.int32)
    on_diag = me_r == me_c
    side = jnp.where(on_diag, 0, 1).astype(jnp.int32)
    nxt_r, nxt_c = _rem(me_r + 1, G), _rem(me_c + 1, G)
    prv_r, prv_c = _rem(me_r + 3, G), _rem(me_c + 3, G)

    loads = [pltpu.make_async_copy(a_hbm.at[:, :, pl.ds(p * 2 * NB, 2 * NB)], mat.at[p], in_sem.at[p]) for p in range(PAIRS)]
    for cp in loads:
        cp.start()
    zero[...] = jnp.zeros_like(zero)

    barrier = pltpu.get_barrier_semaphore()
    for d in range(1, G):
        pl.semaphore_signal(barrier, inc=1, device_id={"row": _rem(me_r + d, G)}, device_id_type=MESH)
        pl.semaphore_signal(barrier, inc=1, device_id={"col": _rem(me_c + d, G)}, device_id_type=MESH)

    @pl.when(on_diag)
    def _():
        pl.semaphore_signal(barrier, inc=1, device_id={"row": nxt_r, "col": nxt_c}, device_id_type=MESH)
        pl.semaphore_signal(barrier, inc=1, device_id={"row": prv_r, "col": prv_c}, device_id_type=MESH)
    pl.semaphore_wait(barrier, jnp.where(on_diag, 8, 6).astype(jnp.int32))
    for cp in loads:
        cp.wait()

    def index(k, q):
        s = _div(k, 8)
        return 40 * s - 4 * s * (s - 1) + (k - 8 * s) * (5 - s) + (q - s)

    def first(k, x):
        s = _div(k, 8)
        return s + jnp.where(8 * s + 4 + x <= k, 1, 0).astype(jnp.int32)

    def half_of(k):
        return pl.multiple_of(_rem(_div(k, 4), 2) * NB, NB)

    def row_copy(k, q, d):
        blk = pan.at[0, index(k, q)]
        return pltpu.make_async_remote_copy(blk, blk, send_sem.at[0], row_sem.at[index(k, q)],
                                            device_id={"col": _rem(me_c + d, G)}, device_id_type=MESH)

    def col_copy(k, q, d):
        i = index(k, q)
        return pltpu.make_async_remote_copy(pan.at[0, i], pan.at[1, i], send_sem.at[1], col_sem.at[i],
                                            device_id={"row": _rem(me_r + d, G)}, device_id_type=MESH)

    def w_copy(k, d):
        return pltpu.make_async_remote_copy(wb.at[k], wb.at[k], send_sem.at[2], w_sem.at[k],
                                            device_id={"row": _rem(me_r + d, G)}, device_id_type=MESH)

    def w_next_copy(k):
        return pltpu.make_async_remote_copy(wb.at[k], wb.at[k], send_sem.at[2], w_sem.at[k],
                                            device_id={"row": nxt_r, "col": nxt_c}, device_id_type=MESH)

    def raw_copy(k):
        src = mat.at[_div(k, 8), _div(k + 1, 4), :, pl.ds(half_of(k), NB)]
        return pltpu.make_async_remote_copy(src, raw.at[k], send_sem.at[3], raw_sem.at[k],
                                            device_id={"col": nxt_c}, device_id_type=MESH)

    def factor_step(k, with_prev):
        @pl.when((me_r == _rem(k, G)) & (me_c == _rem(k, G)))
        def _():
            t = _div(k, 4)
            blk = mat[_div(k, 8), t, :, pl.ds(half_of(k), NB)]
            if with_prev:
                w_next_copy(k - 1).wait_recv()
                raw_copy(k - 1).wait_recv()
                x = _nt(raw[k - 1], wb[k - 1])
                blk = blk - _nt(x, x)
            _factor(blk, ubuf, wb.at[k])

            @pl.when(k < N_STEPS - 1)
            def _():
                w_next_copy(k).start()
                for d in range(1, G):
                    w_copy(k, d).start()
            diag[t] = ubuf[...].T

    def raw_step(k):
        @pl.when((me_c == _rem(k, G)) & (me_r == _rem(k + 1, G)) & (k < N_STEPS - 1))
        def _():
            raw_copy(k).start()

    def panel_step(k):
        @pl.when(me_c == _rem(k, G))
        def _():
            s = _div(k, 8)
            t = _div(k, 4)

            @pl.when((me_r != _rem(k, G)) & (k < N_STEPS - 1))
            def _():
                w_copy(k, 1).wait_recv()

            def block(q, _):
                i = index(k, q)
                a = mat[s, pl.ds(2 * q, 2), :, pl.ds(half_of(k), NB)].reshape(2 * NB, NB)
                pan[0, i] = _nt(a, wb[k])
                for d in range(1, G):
                    row_copy(k, q, d).start()
                return 0
            lax.fori_loop(jnp.where(k < N_STEPS - 1, first(k, me_r), PAIRS), PAIRS, block, 0)

            def tile(ti, _):
                dst = o_hbm.at[ti, :, pl.ds(pl.multiple_of(t * NB, NB), NB)]
                i = 4 * ti + me_r

                @pl.when(i > k)
                def _():
                    src = pan.at[0, index(k, _div(ti, 2)), pl.ds(pl.multiple_of(_rem(ti, 2) * NB, NB), NB), :]
                    pltpu.make_async_copy(src, dst, out_sem).start()

                @pl.when(i == k)
                def _():
                    pltpu.make_async_copy(diag.at[t], dst, out_sem).start()

                @pl.when(i < k)
                def _():
                    pltpu.make_async_copy(zero, dst, out_sem).start()
                return 0
            lax.fori_loop(0, 10, tile, 0)

    def receive_step(k):
        def row_wait(q, _):
            @pl.when(me_c != _rem(k, G))
            def _():
                row_copy(k, q, 1).wait_recv()

            @pl.when(on_diag)
            def _():
                for d in range(1, G):
                    col_copy(k, q, d).start()
            return 0
        lax.fori_loop(first(k, me_r), PAIRS, row_wait, 0)

        @pl.when(jnp.logical_not(on_diag))
        def _():
            def col_wait(q, _):
                col_copy(k, q, 1).wait_recv()
                return 0
            lax.fori_loop(first(k, me_c), PAIRS, col_wait, 0)

    def update(k, p, _):
        right = pan[side, index(k, p)]

        def rows(q, _):
            rs = pl.ds(2 * q, 2)
            prod = _nt(pan[0, index(k, q)], right)
            mat[p, rs] = mat[p, rs] - prod.reshape(2, NB, 2 * NB)
            return 0
        lax.fori_loop(jnp.maximum(p, first(k, me_r)), PAIRS, rows, 0)
        return 0

    raw_step(jnp.int32(0))
    factor_step(jnp.int32(0), False)
    panel_step(jnp.int32(0))

    def step(k, _):
        factor_step(k + 1, True)

        @pl.when((me_c == _rem(k, G)) & (me_r == _rem(k + 1, G)))
        def _():
            raw_copy(k).wait_send()
        receive_step(k)
        next_col = me_c == _rem(k + 1, G)
        p1 = jnp.where(next_col, _div(k + 1, 8), first(k, me_c))

        @pl.when(next_col)
        def _():
            update(k, p1, 0)
        raw_step(k + 1)
        panel_step(k + 1)
        lax.fori_loop(jnp.where(next_col, p1 + 1, p1), PAIRS, lambda p, x: update(k, p, x), 0)
        return 0
    lax.fori_loop(0, N_STEPS - 1, step, 0)

    def drain(k, _):
        mine = me_c == _rem(k, G)

        @pl.when(mine & (me_r == _rem(k, G)))
        def _():
            for d in range(G):
                w_next_copy(k).wait_send()

        def rows(q, _):
            @pl.when(mine)
            def _():
                for d in range(1, G):
                    row_copy(k, q, d).wait_send()

            @pl.when(on_diag)
            def _():
                for d in range(1, G):
                    col_copy(k, q, d).wait_send()
            return 0
        lax.fori_loop(first(k, me_r), PAIRS, rows, 0)
        return 0
    lax.fori_loop(0, N_STEPS - 1, drain, 0)
    pltpu.make_async_copy(o_hbm, o_hbm, out_sem).wait()


def solution(mesh):
    def local(a):
        return pl.pallas_call(
            _kernel,
            out_shape=jax.ShapeDtypeStruct(a.shape, a.dtype),
            in_specs=[pl.BlockSpec(memory_space=pl.ANY)],
            out_specs=pl.BlockSpec(memory_space=pl.ANY),
            scratch_shapes=[
                pltpu.VMEM((PAIRS, 10, NB, 2 * NB), jnp.float32),
                pltpu.VMEM((2, N_BLOCKS, 2 * NB, NB), jnp.float32),
                pltpu.VMEM((N_STEPS, NB, NB), jnp.float32),
                pltpu.VMEM((N_STEPS, NB, NB), jnp.float32),
                pltpu.VMEM((10, NB, NB), jnp.float32),
                pltpu.VMEM((NB, NB), jnp.float32),
                pltpu.VMEM((NB, NB), jnp.float32),
                pltpu.SemaphoreType.DMA((N_BLOCKS,)),
                pltpu.SemaphoreType.DMA((N_BLOCKS,)),
                pltpu.SemaphoreType.DMA((N_STEPS,)),
                pltpu.SemaphoreType.DMA((N_STEPS,)),
                pltpu.SemaphoreType.DMA((4,)),
                pltpu.SemaphoreType.DMA((PAIRS,)),
                pltpu.SemaphoreType.DMA,
            ],
            compiler_params=pltpu.CompilerParams(collective_id=0, has_side_effects=True, vmem_limit_bytes=63 * 1024 * 1024),
            name="cholesky",
        )(a)

    spec = P(("part", "row"), None, "col")
    return jax.shard_map(local, mesh=mesh, in_specs=(spec,), out_specs=spec, check_vma=False)
```
